32 devices in a mesh: part: 1 (over z), tp: 4 (over y), dp: 8 (over x, core).
Axes of the slice: x: 4, y: 4, z: 1, core: 2. Of those that a mesh axis runs over, the one named last changes fastest.
The devices are a block of a 4x4x8 slice.
Arguments:
- hidden: bfloat16 [24, 384, 5120], P(('part', 'dp'))
- ln_scale: float32 [5120], replicated
- w_q: bfloat16 [5120, 5120], P('dp', 'tp')
- w_kv: bfloat16 [5120, 256], P('dp')
- w_gate: bfloat16 [5120, 20480], P('dp', 'tp')
- w_up: bfloat16 [5120, 20480], P('dp', 'tp')
- w_o: bfloat16 [5120, 5120], P('tp', 'dp')
- w_down: bfloat16 [20480, 5120], P('tp', 'dp')
- prompt_len: int32 [24], P(('part', 'dp'))
Outputs:
- output 1: bfloat16 [24, 384, 5120], P(('part', 'dp'))
- output 2: bfloat16 [24, 384, 128], P(('part', 'dp'))
- output 3: bfloat16 [24, 384, 128], P(('part', 'dp'))
All inputs are finite; a program needn't handle non-finite values.
Results may differ from the reference program's by a relative error of at most 0.00937125.
Values are sent between devices in bfloat16 or wider.
A program may use at most 768 MiB of HBM per device.

```python
import jax
import jax.numpy as jnp
from jax import lax

D_MODEL = 5120
NUM_HEADS = 40
HEAD_DIM = 128
FF_DIM = 20480
SEQ_LEN = 384
BATCH_SIZE = 24
LN_EPS = 1e-6
ROPE_BASE = 10000.0
MASK_VALUE = -1e30


def draw_lengths(len_key):
    key_a, key_b = jax.random.split(len_key)
    lengths = jax.random.randint(key_a, (BATCH_SIZE,), SEQ_LEN // 2, SEQ_LEN + 1, jnp.int32)
    long_idx = jax.random.randint(key_b, (), 0, BATCH_SIZE, jnp.int32)
    lengths = lengths.at[long_idx].set(SEQ_LEN)
    lengths = lengths.at[(long_idx + BATCH_SIZE // 2) % BATCH_SIZE].set(SEQ_LEN // 2)
    return lengths.astype(jnp.int32)


def setup_inputs(seed: int = 0, part: int = 0) -> dict:
    base_key = jax.random.key(seed)
    w_keys = jax.random.split(base_key, 7)
    part_keys = jax.random.split(jax.random.fold_in(base_key, part), 2)
    in_gain = D_MODEL ** -0.5
    hidden = jax.random.normal(part_keys[0], (BATCH_SIZE, SEQ_LEN, D_MODEL), jnp.float32)
    ln_scale = 1.0 + 0.3 * jax.random.normal(w_keys[0], (D_MODEL,), jnp.float32)
    w_q = 2.0 * in_gain * jax.random.normal(w_keys[1], (D_MODEL, NUM_HEADS * HEAD_DIM), jnp.float32)
    w_kv = in_gain * jax.random.normal(w_keys[2], (D_MODEL, 2 * HEAD_DIM), jnp.float32)
    w_gate = in_gain * jax.random.normal(w_keys[3], (D_MODEL, FF_DIM), jnp.float32)
    w_up = in_gain * jax.random.normal(w_keys[4], (D_MODEL, FF_DIM), jnp.float32)
    w_o = (NUM_HEADS * HEAD_DIM) ** -0.5 * jax.random.normal(w_keys[5], (NUM_HEADS * HEAD_DIM, D_MODEL), jnp.float32)
    w_down = FF_DIM ** -0.5 * jax.random.normal(w_keys[6], (FF_DIM, D_MODEL), jnp.float32)
    return {
        'hidden': hidden.astype(jnp.bfloat16),
        'ln_scale': ln_scale,
        'w_q': w_q.astype(jnp.bfloat16),
        'w_kv': w_kv.astype(jnp.bfloat16),
        'w_gate': w_gate.astype(jnp.bfloat16),
        'w_up': w_up.astype(jnp.bfloat16),
        'w_o': w_o.astype(jnp.bfloat16),
        'w_down': w_down.astype(jnp.bfloat16),
        'prompt_len': draw_lengths(part_keys[1]),
    }


def layer_norm(hidden, ln_scale):
    x_f = hidden.astype(jnp.float32)
    row_mean = jnp.mean(x_f, axis=-1, keepdims=True)
    centered = x_f - row_mean
    row_var = jnp.mean(centered * centered, axis=-1, keepdims=True)
    return (centered * lax.rsqrt(row_var + LN_EPS) * ln_scale).astype(jnp.bfloat16)


def rope_tables():
    half_dim = HEAD_DIM // 2
    inv_freq = ROPE_BASE ** (-2.0 * jnp.arange(half_dim, dtype=jnp.float32) / HEAD_DIM)
    angles = jnp.arange(SEQ_LEN, dtype=jnp.float32)[:, None] * inv_freq[None, :]
    return jnp.cos(angles), jnp.sin(angles)


def apply_rope(x_in, cos_tab, sin_tab):
    half_dim = x_in.shape[-1] // 2
    x_lo = x_in[..., :half_dim]
    x_hi = x_in[..., half_dim:]
    return jnp.concatenate([x_lo * cos_tab - x_hi * sin_tab, x_hi * cos_tab + x_lo * sin_tab], axis=-1)


def one_sequence(hidden, seq_valid, ln_scale, w_q, w_kv, w_gate, w_up, w_o, w_down):
    normed = layer_norm(hidden, ln_scale)
    q_lin = jnp.dot(normed, w_q, preferred_element_type=jnp.float32).astype(jnp.bfloat16)
    kv_lin = jnp.dot(normed, w_kv, preferred_element_type=jnp.float32).astype(jnp.bfloat16)
    gate_lin = jnp.dot(normed, w_gate, preferred_element_type=jnp.float32).astype(jnp.bfloat16)
    up_lin = jnp.dot(normed, w_up, preferred_element_type=jnp.float32).astype(jnp.bfloat16)
    cos_tab, sin_tab = rope_tables()
    q_heads = q_lin.astype(jnp.float32).reshape(SEQ_LEN, NUM_HEADS, HEAD_DIM)
    q_rot = apply_rope(q_heads, cos_tab[:, None, :], sin_tab[:, None, :]).astype(jnp.bfloat16)
    k_rot = apply_rope(kv_lin[:, :HEAD_DIM].astype(jnp.float32), cos_tab, sin_tab).astype(jnp.bfloat16)
    v_val = kv_lin[:, HEAD_DIM:]
    scores = jnp.einsum('qhd,kd->hqk', q_rot.astype(jnp.float32), k_rot.astype(jnp.float32)) * (HEAD_DIM ** -0.5)
    positions = jnp.arange(SEQ_LEN)
    key_mask = (positions[None, :] <= positions[:, None]) & (positions[None, :] < seq_valid)
    scores = jnp.where(key_mask[None, :, :], scores, MASK_VALUE)
    probs_bf = jax.nn.softmax(scores, axis=-1).astype(jnp.bfloat16)
    attn_out = jnp.einsum('hqk,kd->qhd', probs_bf.astype(jnp.float32), v_val.astype(jnp.float32)).astype(jnp.bfloat16)
    attn_out = attn_out.reshape(SEQ_LEN, NUM_HEADS * HEAD_DIM)
    ffn_act = (jax.nn.silu(gate_lin.astype(jnp.float32)) * up_lin.astype(jnp.float32)).astype(jnp.bfloat16)
    y_sum = jnp.dot(attn_out, w_o, preferred_element_type=jnp.float32) + jnp.dot(ffn_act, w_down, preferred_element_type=jnp.float32)
    out = (hidden.astype(jnp.float32) + y_sum).astype(jnp.bfloat16)
    return out, k_rot, v_val


def reference(hidden, ln_scale, w_q, w_kv, w_gate, w_up, w_o, w_down, prompt_len):
    def per_seq(seq_item):
        return one_sequence(seq_item[0], seq_item[1], ln_scale, w_q, w_kv, w_gate, w_up, w_o, w_down)
    out, k_cache, v_cache = lax.map(per_seq, (hidden, prompt_len))
    return (out, k_cache, v_cache)
```

```python
import functools

import jax
import jax.numpy as jnp
from jax import lax
from jax.experimental import pallas as pl
from jax.experimental.pallas import tpu as pltpu
from jax.sharding import PartitionSpec as P


LN_EPS = 1e-6
ROPE_BASE = 10000.0
MASK_VALUE = -1e30
VMEM_LIMIT = 60 * 1024 * 1024


SIB, PAIR, CUT = 1, 2, 6
OWNERS = (0, PAIR, CUT, CUT ^ PAIR)


def cost(flops, nbytes):
    return pl.CostEstimate(flops=int(flops), bytes_accessed=int(nbytes), transcendentals=0)


def ln_kernel(h_ref, s_ref, u_ref):
    x_f = h_ref[...].astype(jnp.float32)
    row_mean = jnp.mean(x_f, axis=-1, keepdims=True)
    centered = x_f - row_mean
    row_var = jnp.mean(centered * centered, axis=-1, keepdims=True)
    u_ref[...] = (centered * lax.rsqrt(row_var + LN_EPS) * s_ref[...]).astype(jnp.bfloat16)


def layer_norm(h, ln_scale):
    rows, width = h.shape
    tile = 96
    return pl.pallas_call(
        ln_kernel,
        grid=(rows // tile,),
        in_specs=[pl.BlockSpec((tile, width), lambda i: (i, 0)), pl.BlockSpec((1, width), lambda i: (0, 0))],
        out_specs=pl.BlockSpec((tile, width), lambda i: (i, 0)),
        out_shape=jax.ShapeDtypeStruct((rows, width), jnp.bfloat16),
        cost_estimate=cost(8 * rows * width, 4 * rows * width),
        name="norm",
    )(h, ln_scale.reshape(1, width))


def load_rows(dp_ref, blocks, wbuf, sem):
    depth = blocks[0].shape[0]
    copies = []
    for j, mask in enumerate(m ^ c for m in OWNERS for c in (0, SIB)):
        start = pl.multiple_of((dp_ref[0] ^ mask) * depth, depth)
        copies.append(pltpu.make_async_copy(blocks[j], wbuf.at[pl.ds(start, depth), :], sem.at[j]))
    for c in copies:
        c.start()
    for c in copies:
        c.wait()


def qkv_kernel(head_dim, seq_len, dp_ref, len_ref, u_ref, cos_ref, sin_ref, *refs):
    blocks, (o_ref, k_ref, v_ref, wbuf, sem) = refs[:8], refs[-5:]

    @pl.when(pl.program_id(0) == 0)
    def _():
        load_rows(dp_ref, blocks, wbuf, sem)

    n_valid = len_ref[pl.program_id(0)]
    half = head_dim // 2
    q_width = wbuf.shape[1] - 2 * head_dim
    z = jnp.dot(u_ref[...], wbuf[...], preferred_element_type=jnp.float32).astype(jnp.bfloat16)
    cos_t, sin_t = cos_ref[...], sin_ref[...]

    def rope(x_bf):
        x = x_bf.astype(jnp.float32)
        return (x * cos_t + pltpu.roll(x, half, 1) * sin_t).astype(jnp.bfloat16)

    k_rot = rope(z[:, q_width:q_width + head_dim])
    v_val = z[:, q_width + head_dim:]
    k_ref[...] = k_rot
    v_ref[...] = v_val
    rows = lax.broadcasted_iota(jnp.int32, (seq_len, seq_len), 0)
    cols = lax.broadcasted_iota(jnp.int32, (seq_len, seq_len), 1)
    live = (cols <= rows) & (cols < n_valid)
    for h in range(q_width // head_dim):
        q_rot = rope(z[:, h * head_dim:(h + 1) * head_dim])
        s = lax.dot_general(q_rot, k_rot, (((1,), (1,)), ((), ())), preferred_element_type=jnp.float32)
        s = jnp.where(live, s * (head_dim ** -0.5), MASK_VALUE)
        e = jnp.exp(s - jnp.max(s, axis=-1, keepdims=True))
        p = (e * (1.0 / jnp.sum(e, axis=-1, keepdims=True))).astype(jnp.bfloat16)
        o = jnp.dot(p, v_val, preferred_element_type=jnp.float32)
        o_ref[:, h * head_dim:(h + 1) * head_dim] = o.astype(jnp.bfloat16)


def qkv_attend(dp, lens, u, cos_t, sin_t, blocks, head_dim, seq_len, mixed_width, mixed=None):
    rows, width = u.shape
    _, cols = blocks[0].shape
    q_width = cols - 2 * head_dim
    whole = lambda shape: pl.BlockSpec(shape, lambda i: (0, 0))
    smem = pl.BlockSpec(memory_space=pltpu.SMEM)
    later = mixed is not None
    first = rows // seq_len if later else 0
    return pl.pallas_call(
        functools.partial(qkv_kernel, head_dim, seq_len),
        grid=(rows // seq_len,),
        in_specs=[smem, smem, pl.BlockSpec((seq_len, width), lambda i: (i, 0)),
                  whole((seq_len, head_dim)), whole((seq_len, head_dim))] + [pl.BlockSpec(memory_space=pl.ANY)] * (8 + later),
        out_specs=[pl.BlockSpec((seq_len, q_width), lambda i: (first + i, 0)),
                   pl.BlockSpec((seq_len, head_dim), lambda i: (i, 0)),
                   pl.BlockSpec((seq_len, head_dim), lambda i: (i, 0))],
        out_shape=[jax.ShapeDtypeStruct((2 * rows, mixed_width), jnp.bfloat16),
                   jax.ShapeDtypeStruct((rows, head_dim), jnp.bfloat16),
                   jax.ShapeDtypeStruct((rows, head_dim), jnp.bfloat16)],
        scratch_shapes=[pltpu.VMEM((width, cols), jnp.bfloat16), pltpu.SemaphoreType.DMA((8,))],
        input_output_aliases={13: 0} if later else {},
        compiler_params=pltpu.CompilerParams(vmem_limit_bytes=VMEM_LIMIT),
        cost_estimate=cost(2 * rows * width * cols * 2, 2 * (rows * width + width * cols)),
        name="qkv",
    )(dp, lens, u, cos_t, sin_t, *blocks, *([mixed] if later else []))


def ffn_kernel(steps, dp_ref, u0, u1, *refs):
    blocks, (_, a_ref, wbuf, ubuf, sem, usem) = refs[:8], refs[8:]
    i = pl.program_id(0)
    tile = ubuf.shape[1]

    def fetch(step):
        row = pl.multiple_of(lax.rem(step, steps) * tile, tile)
        slot = lax.rem(step, 2)
        for j, u in enumerate((u0, u1)):
            @pl.when(step // steps == j)
            def _(u=u):
                pltpu.make_async_copy(u.at[pl.ds(row, tile), :], ubuf.at[slot], usem.at[slot]).start()

    @pl.when(i == 0)
    def _():
        fetch(i)
        load_rows(dp_ref, blocks, wbuf, sem)

    @pl.when(i + 1 < 2 * steps)
    def _():
        fetch(i + 1)

    slot = lax.rem(i, 2)
    pltpu.make_async_copy(u0.at[pl.ds(0, tile), :], ubuf.at[slot], usem.at[slot]).wait()
    n = a_ref.shape[1]
    z = jnp.dot(ubuf[slot], wbuf[...], preferred_element_type=jnp.float32).astype(jnp.bfloat16)
    g, p = z[:, :n].astype(jnp.float32), z[:, n:].astype(jnp.float32)
    a_ref[...] = (g * jax.nn.sigmoid(g) * p).astype(jnp.bfloat16)


def ffn_chunk(dp, u_own, u_pair, blocks, mixed, place):
    rows, width = u_own.shape
    cols = blocks[0].shape[1]
    steps = 2
    tile, n = rows // steps, cols // 2
    anywhere = pl.BlockSpec(memory_space=pl.ANY)
    return pl.pallas_call(
        functools.partial(ffn_kernel, steps),
        grid=(2 * steps,),
        in_specs=[pl.BlockSpec(memory_space=pltpu.SMEM)] + [anywhere] * 11,
        out_specs=pl.BlockSpec((tile, n), lambda i: (i, place)),
        out_shape=jax.ShapeDtypeStruct(mixed.shape, mixed.dtype),
        scratch_shapes=[pltpu.VMEM((width, cols), jnp.bfloat16), pltpu.VMEM((2, tile, width), jnp.bfloat16),
                        pltpu.SemaphoreType.DMA((8,)), pltpu.SemaphoreType.DMA((2,))],
        input_output_aliases={11: 0},
        compiler_params=pltpu.CompilerParams(vmem_limit_bytes=VMEM_LIMIT),
        cost_estimate=cost(4 * rows * width * cols, 2 * (2 * rows * width + width * cols)),
        name="ffn",
    )(dp, u_own, u_pair, *blocks, mixed)


def down_kernel(steps, joint, core_ref, x_ref, w0, w1, *refs):
    both_ref, solo_ref, wbuf, sem = refs[-4:]
    i = pl.program_id(0)

    @pl.when(i == 0)
    def _():
        n = w0.shape[1]
        copies = []
        for j, w in enumerate((w0, w1)):
            start = pl.multiple_of((core_ref[0] ^ j) * n, n)
            copies.append(pltpu.make_async_copy(w, wbuf.at[:, pl.ds(start, n)], sem.at[j]))
        for c in copies:
            c.start()
        for c in copies:
            c.wait()

    y = jnp.dot(x_ref[...], wbuf[...], preferred_element_type=jnp.float32).astype(jnp.bfloat16)

    @pl.when(i // steps == joint)
    def _():
        both_ref[...] = y

    @pl.when(i // steps != joint)
    def _():
        solo_ref[...] = y


def down_block(core, mixed, w0, w1, both=None):
    depth = mixed.shape[1]
    n = w0.shape[1]
    rows, steps = mixed.shape[0] // 2, 2
    tile = rows // steps
    joint = 0 if both is None else 1
    first = joint * steps
    anywhere = pl.BlockSpec(memory_space=pl.ANY)
    hold = lambda i, start: jnp.clip(i - start, 0, steps - 1)
    return pl.pallas_call(
        functools.partial(down_kernel, steps, joint),
        grid=(2 * steps,),
        in_specs=[pl.BlockSpec(memory_space=pltpu.SMEM), pl.BlockSpec((tile, depth), lambda i: (i, 0))]
        + [anywhere] * (2 + joint),
        out_specs=[pl.BlockSpec((tile, 2 * n), lambda i: (first + hold(i, first), 0)),
                   pl.BlockSpec((tile, 2 * n), lambda i: (hold(i, steps - first), 0))],
        out_shape=[jax.ShapeDtypeStruct((2 * rows, 2 * n), jnp.bfloat16), jax.ShapeDtypeStruct((rows, 2 * n), jnp.bfloat16)],
        scratch_shapes=[pltpu.VMEM((depth, 2 * n), jnp.bfloat16), pltpu.SemaphoreType.DMA((2,))],
        input_output_aliases={4: 0} if joint else {},
        compiler_params=pltpu.CompilerParams(vmem_limit_bytes=VMEM_LIMIT),
        cost_estimate=cost(8 * rows * depth * n, 4 * (rows * depth + depth * n + 2 * rows * n)),
        name="down",
    )(core, mixed, w0, w1, *([] if both is None else [both]))


def solution(mesh):
    n_dp, n_tp = mesh.shape['dp'], mesh.shape['tp']
    batch_spec = P(('part', 'dp'), None, None)

    def swap(x, mask):
        return lax.ppermute(x, 'dp', [(i, i ^ mask) for i in range(n_dp)])

    def local_layer(hidden, ln_scale, w_q, w_kv, w_gate, w_up, w_o, w_down, prompt_len):
        n_seq, seq_len, width = hidden.shape
        rows = n_seq * seq_len
        head_dim = w_kv.shape[1] // 2
        q_half, f_half = w_q.shape[1] // 2, w_gate.shape[1] // 2
        out_cols = w_o.shape[1]
        n_ffn = f_half // q_half
        dp, tp = lax.axis_index('dp'), lax.axis_index('tp')
        core, chip = dp % 2, dp // 2
        mine = ((chip + 1) // 2) % 2
        dp_arr, core_arr = dp.reshape(1).astype(jnp.int32), core.reshape(1).astype(jnp.int32)

        def in_chunk(k, half):
            if k == 0:
                return jnp.concatenate([lax.dynamic_slice_in_dim(w_q, half * q_half, q_half, 1), w_kv], axis=1)
            start = half * f_half + (k - 1) * q_half
            return jnp.concatenate([lax.dynamic_slice_in_dim(w_gate, start, q_half, 1),
                                    lax.dynamic_slice_in_dim(w_up, start, q_half, 1)], axis=1)

        def out_chunk(half):
            return jnp.concatenate([lax.dynamic_slice_in_dim(w_o, half * q_half, q_half, 0),
                                    lax.dynamic_slice_in_dim(w_down, half * f_half, f_half, 0)], axis=0)

        def gather(make):
            own, other = lax.optimization_barrier((make(mine), make(1 - mine)))
            cut = swap(own, CUT)
            pair = swap(other, PAIR)
            relay = swap(pair, CUT)
            blocks = []
            for b in (own, pair, cut, relay):
                blocks += [b, swap(b, SIB)]
            return blocks

        chunks = [gather(functools.partial(in_chunk, k)) for k in range(n_ffn + 1)]
        outs = gather(out_chunk)

        h_own = hidden.reshape(rows, width)
        quarter = rows // n_tp
        h_quarter = lax.dynamic_slice_in_dim(h_own, tp * quarter, quarter, 0)
        u_quarter = layer_norm(h_quarter, ln_scale)
        u_own = layer_norm(h_own, ln_scale)
        u_quarter = swap(u_quarter, PAIR)
        u_pair = lax.all_gather(u_quarter, 'tp', axis=0, tiled=True)
        len_pair = swap(prompt_len, PAIR)

        half_dim = head_dim // 2
        inv_freq = ROPE_BASE ** (-2.0 * jnp.arange(half_dim, dtype=jnp.float32) / head_dim)
        angles = jnp.arange(seq_len, dtype=jnp.float32)[:, None] * inv_freq[None, :]
        cos_t, sin_t = jnp.cos(angles), jnp.sin(angles)
        cos_t = jnp.concatenate([cos_t, cos_t], axis=1)
        sin_t = jnp.concatenate([-sin_t, sin_t], axis=1)

        mixed_width = q_half + f_half
        attend = lambda lens, u, *mixed: qkv_attend(
            dp_arr, lens, u, cos_t, sin_t, chunks[0], head_dim, seq_len, mixed_width, *mixed)
        mixed, k_rot, v_val = attend(prompt_len, u_own)
        mixed, _, _ = attend(len_pair, u_pair, mixed)
        for k in range(1, n_ffn + 1):
            mixed = ffn_chunk(dp_arr, u_own, u_pair, chunks[k], mixed, k)

        f32 = jnp.float32
        n_cols = 2 * out_cols
        out = jnp.zeros((rows, width), jnp.bfloat16)
        odd = chip % 2
        h_last = h_quarter
        for j in (0, 2):
            both, to_pair = down_block(core_arr, mixed, outs[2 * j], outs[2 * j + 1])
            both, own = down_block(core_arr, mixed, outs[2 * j + 2], outs[2 * j + 3], both)
            other = swap(to_pair, PAIR)
            part = lax.psum_scatter(both.reshape(2, rows, n_cols), 'tp', scatter_dimension=1, tiled=True)
            moved = swap(part[1], PAIR)
            single = lax.psum_scatter((own.astype(f32) + other.astype(f32)).astype(jnp.bfloat16), 'tp',
                                      scatter_dimension=0, tiled=True)
            y_a = part[0].astype(f32) + moved.astype(f32)
            y_b = single.astype(f32)
            swapped = odd if j == 0 else 1 - odd
            y_slab = jnp.where(swapped == 0, jnp.concatenate([y_a, y_b], axis=1), jnp.concatenate([y_b, y_a], axis=1))
            col = (((chip ^ (OWNERS[j] // 2)) // 2) * (2 * n_cols)).astype(jnp.int32)
            slab = (lax.dynamic_slice_in_dim(h_last, col, 2 * n_cols, 1).astype(f32) + y_slab).astype(jnp.bfloat16)
            slab, h_last = lax.optimization_barrier((slab, h_last))
            full = lax.all_gather(slab, 'tp', axis=0, tiled=True)
            out = lax.dynamic_update_slice_in_dim(out, full, col, 1)
        return (out.reshape(n_seq, seq_len, width), k_rot.reshape(n_seq, seq_len, head_dim),
                v_val.reshape(n_seq, seq_len, head_dim))

    return jax.shard_map(
        local_layer,
        mesh=mesh,
        in_specs=(batch_spec, P(None), P('dp', 'tp'), P('dp', None), P('dp', 'tp'), P('dp', 'tp'), P('tp', 'dp'), P('tp', 'dp'), P(('part', 'dp'))),
        out_specs=(batch_spec, batch_spec, batch_spec),
        check_vma=False,
    )
```

```python
import functools

import jax
import jax.numpy as jnp
from jax import lax
from jax.experimental import pallas as pl
from jax.experimental.pallas import tpu as pltpu
from jax.sharding import PartitionSpec as P


LN_EPS = 1e-6
ROPE_BASE = 10000.0
MASK_VALUE = -1e30
VMEM_LIMIT = 60 * 1024 * 1024


SIB, PAIR, CUT = 1, 2, 6
OWNERS = (0, PAIR, CUT, CUT ^ PAIR)


def cost(flops, nbytes):
    return pl.CostEstimate(flops=int(flops), bytes_accessed=int(nbytes), transcendentals=0)


def ln_kernel(h_ref, s_ref, u_ref):
    x_f = h_ref[...].astype(jnp.float32)
    row_mean = jnp.mean(x_f, axis=-1, keepdims=True)
    centered = x_f - row_mean
    row_var = jnp.mean(centered * centered, axis=-1, keepdims=True)
    u_ref[...] = (centered * lax.rsqrt(row_var + LN_EPS) * s_ref[...]).astype(jnp.bfloat16)


def layer_norm(h, ln_scale):
    rows, width = h.shape
    tile = 96
    return pl.pallas_call(
        ln_kernel,
        grid=(rows // tile,),
        in_specs=[pl.BlockSpec((tile, width), lambda i: (i, 0)), pl.BlockSpec((1, width), lambda i: (0, 0))],
        out_specs=pl.BlockSpec((tile, width), lambda i: (i, 0)),
        out_shape=jax.ShapeDtypeStruct((rows, width), jnp.bfloat16),
        cost_estimate=cost(8 * rows * width, 4 * rows * width),
        name="norm",
    )(h, ln_scale.reshape(1, width))


def load_rows(dp_ref, blocks, wbuf, sem):
    depth = blocks[0].shape[0]
    copies = []
    for j, mask in enumerate(m ^ c for m in OWNERS for c in (0, SIB)):
        start = pl.multiple_of((dp_ref[0] ^ mask) * depth, depth)
        copies.append(pltpu.make_async_copy(blocks[j], wbuf.at[pl.ds(start, depth), :], sem.at[j]))
    for c in copies:
        c.start()
    for c in copies:
        c.wait()


def qkv_kernel(head_dim, seq_len, dp_ref, len_ref, u_ref, cos_ref, sin_ref, *refs):
    blocks, (o_ref, k_ref, v_ref, wbuf, sem) = refs[:8], refs[-5:]

    @pl.when(pl.program_id(0) == 0)
    def _():
        load_rows(dp_ref, blocks, wbuf, sem)

    n_valid = len_ref[pl.program_id(0)]
    half = head_dim // 2
    q_width = wbuf.shape[1] - 2 * head_dim
    z = jnp.dot(u_ref[...], wbuf[...], preferred_element_type=jnp.float32).astype(jnp.bfloat16)
    cos_t, sin_t = cos_ref[...], sin_ref[...]

    def rope(x_bf):
        x = x_bf.astype(jnp.float32)
        return (x * cos_t + pltpu.roll(x, half, 1) * sin_t).astype(jnp.bfloat16)

    k_rot = rope(z[:, q_width:q_width + head_dim])
    v_val = z[:, q_width + head_dim:]
    k_ref[...] = k_rot
    v_ref[...] = v_val
    rows = lax.broadcasted_iota(jnp.int32, (seq_len, seq_len), 0)
    cols = lax.broadcasted_iota(jnp.int32, (seq_len, seq_len), 1)
    live = (cols <= rows) & (cols < n_valid)
    for h in range(q_width // head_dim):
        q_rot = rope(z[:, h * head_dim:(h + 1) * head_dim])
        s = lax.dot_general(q_rot, k_rot, (((1,), (1,)), ((), ())), preferred_element_type=jnp.float32)
        s = jnp.where(live, s * (head_dim ** -0.5), MASK_VALUE)
        e = jnp.exp(s - jnp.max(s, axis=-1, keepdims=True))
        p = (e * (1.0 / jnp.sum(e, axis=-1, keepdims=True))).astype(jnp.bfloat16)
        o = jnp.dot(p, v_val, preferred_element_type=jnp.float32)
        o_ref[:, h * head_dim:(h + 1) * head_dim] = o.astype(jnp.bfloat16)


def qkv_attend(dp, lens, u, cos_t, sin_t, blocks, head_dim, seq_len, mixed_width, mixed=None):
    rows, width = u.shape
    _, cols = blocks[0].shape
    q_width = cols - 2 * head_dim
    whole = lambda shape: pl.BlockSpec(shape, lambda i: (0, 0))
    smem = pl.BlockSpec(memory_space=pltpu.SMEM)
    later = mixed is not None
    first = rows // seq_len if later else 0
    return pl.pallas_call(
        functools.partial(qkv_kernel, head_dim, seq_len),
        grid=(rows // seq_len,),
        in_specs=[smem, smem, pl.BlockSpec((seq_len, width), lambda i: (i, 0)),
                  whole((seq_len, head_dim)), whole((seq_len, head_dim))] + [pl.BlockSpec(memory_space=pl.ANY)] * (8 + later),
        out_specs=[pl.BlockSpec((seq_len, q_width), lambda i: (first + i, 0)),
                   pl.BlockSpec((seq_len, head_dim), lambda i: (i, 0)),
                   pl.BlockSpec((seq_len, head_dim), lambda i: (i, 0))],
        out_shape=[jax.ShapeDtypeStruct((2 * rows, mixed_width), jnp.bfloat16),
                   jax.ShapeDtypeStruct((rows, head_dim), jnp.bfloat16),
                   jax.ShapeDtypeStruct((rows, head_dim), jnp.bfloat16)],
        scratch_shapes=[pltpu.VMEM((width, cols), jnp.bfloat16), pltpu.SemaphoreType.DMA((8,))],
        input_output_aliases={13: 0} if later else {},
        compiler_params=pltpu.CompilerParams(vmem_limit_bytes=VMEM_LIMIT),
        cost_estimate=cost(2 * rows * width * cols * 2, 2 * (rows * width + width * cols)),
        name="qkv",
    )(dp, lens, u, cos_t, sin_t, *blocks, *([mixed] if later else []))


def ffn_kernel(steps, dp_ref, u0, u1, *refs):
    blocks, (_, a_ref, wbuf, ubuf, sem, usem) = refs[:8], refs[8:]
    i = pl.program_id(0)
    tile = ubuf.shape[1]

    def fetch(step):
        row = pl.multiple_of(lax.rem(step, steps) * tile, tile)
        slot = lax.rem(step, 2)
        for j, u in enumerate((u0, u1)):
            @pl.when(step // steps == j)
            def _(u=u):
                pltpu.make_async_copy(u.at[pl.ds(row, tile), :], ubuf.at[slot], usem.at[slot]).start()

    @pl.when(i == 0)
    def _():
        fetch(i)
        load_rows(dp_ref, blocks, wbuf, sem)

    @pl.when(i + 1 < 2 * steps)
    def _():
        fetch(i + 1)

    slot = lax.rem(i, 2)
    pltpu.make_async_copy(u0.at[pl.ds(0, tile), :], ubuf.at[slot], usem.at[slot]).wait()
    n = a_ref.shape[1]
    z = jnp.dot(ubuf[slot], wbuf[...], preferred_element_type=jnp.float32).astype(jnp.bfloat16)
    g, p = z[:, :n].astype(jnp.float32), z[:, n:].astype(jnp.float32)
    a_ref[...] = (g * jax.nn.sigmoid(g) * p).astype(jnp.bfloat16)


def ffn_chunk(dp, u_own, u_pair, blocks, mixed, place):
    rows, width = u_own.shape
    cols = blocks[0].shape[1]
    steps = 2
    tile, n = rows // steps, cols // 2
    anywhere = pl.BlockSpec(memory_space=pl.ANY)
    return pl.pallas_call(
        functools.partial(ffn_kernel, steps),
        grid=(2 * steps,),
        in_specs=[pl.BlockSpec(memory_space=pltpu.SMEM)] + [anywhere] * 11,
        out_specs=pl.BlockSpec((tile, n), lambda i: (i, place)),
        out_shape=jax.ShapeDtypeStruct(mixed.shape, mixed.dtype),
        scratch_shapes=[pltpu.VMEM((width, cols), jnp.bfloat16), pltpu.VMEM((2, tile, width), jnp.bfloat16),
                        pltpu.SemaphoreType.DMA((8,)), pltpu.SemaphoreType.DMA((2,))],
        input_output_aliases={11: 0},
        compiler_params=pltpu.CompilerParams(vmem_limit_bytes=VMEM_LIMIT),
        cost_estimate=cost(4 * rows * width * cols, 2 * (2 * rows * width + width * cols)),
        name="ffn",
    )(dp, u_own, u_pair, *blocks, mixed)


def down_kernel(core_ref, x_ref, w0, w1, *refs):
    y_ref, wbuf, sem = refs[-3:]

    @pl.when(pl.program_id(0) == 0)
    def _():
        n = w0.shape[1]
        copies = []
        for j, w in enumerate((w0, w1)):
            start = pl.multiple_of((core_ref[0] ^ j) * n, n)
            copies.append(pltpu.make_async_copy(w, wbuf.at[:, pl.ds(start, n)], sem.at[j]))
        for c in copies:
            c.start()
        for c in copies:
            c.wait()

    y_ref[...] = jnp.dot(x_ref[...], wbuf[...], preferred_element_type=jnp.float32).astype(jnp.bfloat16)


def down_block(core, mixed, token_set, weights, out_sets=1, out_set=0, dest=None):
    depth = mixed.shape[1]
    n = weights[0].shape[1]
    rows, steps = mixed.shape[0] // 2, 2
    tile = rows // steps
    given = [] if dest is None else [dest]
    anywhere = pl.BlockSpec(memory_space=pl.ANY)
    return pl.pallas_call(
        down_kernel,
        grid=(steps,),
        in_specs=[pl.BlockSpec(memory_space=pltpu.SMEM), pl.BlockSpec((tile, depth), lambda i: (token_set * steps + i, 0))]
        + [anywhere] * (2 + len(given)),
        out_specs=pl.BlockSpec((tile, 2 * n), lambda i: (out_set * steps + i, 0)),
        out_shape=jax.ShapeDtypeStruct((out_sets * rows, 2 * n), jnp.bfloat16),
        scratch_shapes=[pltpu.VMEM((depth, 2 * n), jnp.bfloat16), pltpu.SemaphoreType.DMA((2,))],
        input_output_aliases={4: 0} if given else {},
        compiler_params=pltpu.CompilerParams(vmem_limit_bytes=VMEM_LIMIT),
        cost_estimate=cost(4 * rows * depth * n, 2 * (rows * depth + 2 * depth * n + 2 * rows * n)),
        name="down",
    )(core, mixed, *weights, *given)


def place_kernel(at_ref, *refs):
    pieces, (out_ref, sem) = refs[:5], refs[-2:]
    quarter, cols = pieces[3].shape
    copies = []
    for k, (mask, start) in enumerate(((0, 0), (1, 0), (3, 0), (2, 0), (2, cols))):
        row = pl.multiple_of((at_ref[0] ^ mask) * quarter, quarter)
        col = pl.multiple_of(at_ref[1] + start, cols)
        copies.append(pltpu.make_async_copy(
            pieces[k], out_ref.at[pl.ds(row, quarter), pl.ds(col, pieces[k].shape[1])], sem.at[k]))
    for c in copies:
        c.start()
    for c in copies:
        c.wait()


def place(at, pieces, n_tp, width, out=None):
    quarter = pieces[0].shape[0]
    given = [] if out is None else [out]
    anywhere = pl.BlockSpec(memory_space=pl.ANY)
    return pl.pallas_call(
        place_kernel,
        in_specs=[pl.BlockSpec(memory_space=pltpu.SMEM)] + [pl.BlockSpec(memory_space=pltpu.VMEM)] * 5
        + [anywhere] * len(given),
        out_specs=anywhere,
        out_shape=jax.ShapeDtypeStruct((n_tp * quarter, width), jnp.bfloat16),
        scratch_shapes=[pltpu.SemaphoreType.DMA((5,))],
        input_output_aliases={6: 0} if given else {},
        compiler_params=pltpu.CompilerParams(vmem_limit_bytes=VMEM_LIMIT),
        cost_estimate=cost(quarter * width, 4 * quarter * width),
        name="place",
    )(at, *pieces, *given)


def solution(mesh):
    n_dp, n_tp = mesh.shape['dp'], mesh.shape['tp']
    batch_spec = P(('part', 'dp'), None, None)

    def swap(x, mask):
        return lax.ppermute(x, 'dp', [(i, i ^ mask) for i in range(n_dp)])

    def swap_tp(x, mask):
        return lax.ppermute(x, 'tp', [(i, i ^ mask) for i in range(n_tp)])

    def local_layer(hidden, ln_scale, w_q, w_kv, w_gate, w_up, w_o, w_down, prompt_len):
        n_seq, seq_len, width = hidden.shape
        rows = n_seq * seq_len
        head_dim = w_kv.shape[1] // 2
        q_half, f_half = w_q.shape[1] // 2, w_gate.shape[1] // 2
        out_cols = w_o.shape[1]
        n_ffn = f_half // q_half
        dp, tp = lax.axis_index('dp'), lax.axis_index('tp')
        core, chip = dp % 2, dp // 2
        mine = ((chip + 1) // 2) % 2
        dp_arr, core_arr = dp.reshape(1).astype(jnp.int32), core.reshape(1).astype(jnp.int32)

        def in_chunk(k, half):
            if k == 0:
                return jnp.concatenate([lax.dynamic_slice_in_dim(w_q, half * q_half, q_half, 1), w_kv], axis=1)
            start = half * f_half + (k - 1) * q_half
            return jnp.concatenate([lax.dynamic_slice_in_dim(w_gate, start, q_half, 1),
                                    lax.dynamic_slice_in_dim(w_up, start, q_half, 1)], axis=1)

        def out_chunk(half):
            return jnp.concatenate([lax.dynamic_slice_in_dim(w_o, half * q_half, q_half, 0),
                                    lax.dynamic_slice_in_dim(w_down, half * f_half, f_half, 0)], axis=0)

        def gather(make):
            own, other = lax.optimization_barrier((make(mine), make(1 - mine)))
            cut = swap(own, CUT)
            pair = swap(other, PAIR)
            relay = swap(pair, CUT)
            blocks = []
            for b in (own, pair, cut, relay):
                blocks += [b, swap(b, SIB)]
            return blocks

        chunks = [gather(functools.partial(in_chunk, k)) for k in range(n_ffn + 1)]
        outs = gather(out_chunk)

        h_own = hidden.reshape(rows, width)
        quarter = rows // n_tp
        h_quarter = lax.dynamic_slice_in_dim(h_own, tp * quarter, quarter, 0)
        u_quarter = layer_norm(h_quarter, ln_scale)
        u_own = layer_norm(h_own, ln_scale)
        u_quarter = swap(u_quarter, PAIR)
        u_pair = lax.all_gather(u_quarter, 'tp', axis=0, tiled=True)
        len_pair = swap(prompt_len, PAIR)

        half_dim = head_dim // 2
        inv_freq = ROPE_BASE ** (-2.0 * jnp.arange(half_dim, dtype=jnp.float32) / head_dim)
        angles = jnp.arange(seq_len, dtype=jnp.float32)[:, None] * inv_freq[None, :]
        cos_t, sin_t = jnp.cos(angles), jnp.sin(angles)
        cos_t = jnp.concatenate([cos_t, cos_t], axis=1)
        sin_t = jnp.concatenate([-sin_t, sin_t], axis=1)

        mixed_width = q_half + f_half
        attend = lambda lens, u, *mixed: qkv_attend(
            dp_arr, lens, u, cos_t, sin_t, chunks[0], head_dim, seq_len, mixed_width, *mixed)
        mixed, k_rot, v_val = attend(prompt_len, u_own)
        mixed, _, _ = attend(len_pair, u_pair, mixed)
        for k in range(1, n_ffn + 1):
            mixed = ffn_chunk(dp_arr, u_own, u_pair, chunks[k], mixed, k)

        f32 = jnp.float32
        n_cols = 2 * out_cols
        out = None
        odd = chip % 2
        h_last = h_quarter
        for j in (0, 2):
            first, second = outs[2 * j:2 * j + 2], outs[2 * j + 2:2 * j + 4]
            to_pair = down_block(core_arr, mixed, 1, first)
            other = swap(to_pair, PAIR)
            both = down_block(core_arr, mixed, 0, first, 2, 0)
            both = down_block(core_arr, mixed, 1, second, 2, 1, both)
            own = down_block(core_arr, mixed, 0, second)
            part = lax.psum_scatter(both.reshape(2, rows, n_cols), 'tp', scatter_dimension=1, tiled=True)
            moved = swap(part[1], PAIR)
            joined = (own.astype(f32) + other.astype(f32)).astype(jnp.bfloat16)
            single = lax.psum_scatter(joined, 'tp', scatter_dimension=0, tiled=True)
            y_a = part[0].astype(f32) + moved.astype(f32)
            y_b = single.astype(f32)
            swapped = odd if j == 0 else 1 - odd
            y_slab = jnp.where(swapped == 0, jnp.concatenate([y_a, y_b], axis=1), jnp.concatenate([y_b, y_a], axis=1))
            col = (((chip ^ (OWNERS[j] // 2)) // 2) * (2 * n_cols)).astype(jnp.int32)
            slab = (lax.dynamic_slice_in_dim(h_last, col, 2 * n_cols, 1).astype(f32) + y_slab).astype(jnp.bfloat16)
            slab, h_last = lax.optimization_barrier((slab, h_last))
            from_1 = swap_tp(slab, 1)
            from_3 = swap_tp(slab, 3)
            far_lo = swap_tp(from_1[:, :n_cols], 3)
            far_hi = swap_tp(from_3[:, n_cols:], 1)
            at = jnp.stack([tp.astype(jnp.int32), col])
            out = place(at, (slab, from_1, from_3, far_lo, far_hi), n_tp, width, out)
        return (out.reshape(n_seq, seq_len, width), k_rot.reshape(n_seq, seq_len, head_dim),
                v_val.reshape(n_seq, seq_len, head_dim))

    return jax.shard_map(
        local_layer,
        mesh=mesh,
        in_specs=(batch_spec, P(None), P('dp', 'tp'), P('dp', None), P('dp', 'tp'), P('dp', 'tp'), P('tp', 'dp'), P('tp', 'dp'), P(('part', 'dp'))),
        out_specs=(batch_spec, batch_spec, batch_spec),
        check_vma=False,
    )
```
